256 devices in a mesh: row: 16 (over x_lo, y, core), col: 16 (over x_hi, z).
Axes of the slice: x: 4 (x_hi: 2, x_lo: 2; x = x_hi * 2 + x_lo), y: 4, z: 8, core: 2. Of those that a mesh axis runs over, the one named last changes fastest.
Arguments:
- node_features: bfloat16 [262144, 128], P(('row', 'col')), may hold values from -6 to 6
- src_norm: float32 [262144], P(('row', 'col')), may hold values from 0.05 to 1
- dst_norm: float32 [16, 16384], P('col', 'row'), may hold values from 0.1 to 1
- tiles: bfloat16 [16, 16, 320, 128, 128], P('row', 'col'), may hold values from 0 to 0.049804688
- row_block: int32 [16, 16, 320], P('row', 'col'), may hold values from 0 to 127
- col_block: int32 [16, 16, 320], P('row', 'col'), may hold values from 0 to 127
- tile_count: int32 [16, 16], P('row', 'col'), may hold values from 40 to 320, as said below
- weight: bfloat16 [128, 128], replicated, may hold values from -0.5 to 0.5
- bias: float32 [128], replicated, may hold values from -3 to 3
Outputs:
- result: bfloat16 [16, 16384, 128], P('col', 'row')
The draws below stay inside these ranges and needn't reach their ends.
Inputs may be any that keep to these rules, and one draw needn't show every extreme that they name: Slots at or beyond a grid cell's tile_count are ignored (their ids are 0); the live slots of one grid cell name distinct (row_block, col_block) pairs; some grid cell has all 320 slots live.
All inputs are finite; a program needn't handle non-finite values.
Results may differ from the reference program's by a relative error of at most 0.0095.
Values may be sent and summed in bfloat16 or wider, within the bound.
No kernel may reach another device: no remote copies, remote signals or barrier semaphores. Data moves between devices by JAX's collectives and lax.ppermute only.
A program may use at most 128 MiB of HBM per device.

```python
import math
import jax
import jax.numpy as jnp
from jax import lax

TB = 128
F = 128
SB = 128
TILES_DEV = 320
DB = 128
NODES = 262144
N_ROW = 16
N_COL = 16


def tile_layout(key):
    base_key = jax.random.fold_in(key, 7)
    perm_key, shift_key, pick_key = jax.random.split(base_key, 3)
    device_keys = jax.random.split(perm_key, N_ROW * N_COL)
    chosen = jax.vmap(lambda one_key: jax.random.permutation(one_key, DB * SB)[:TILES_DEV])(device_keys)
    chosen = chosen.reshape(N_ROW, N_COL, TILES_DEV).astype(jnp.int32)
    shifts = jax.random.randint(shift_key, (N_ROW * N_COL,), 0, 4, dtype=jnp.int32)
    top_device = jax.random.randint(pick_key, (), 0, N_ROW * N_COL, dtype=jnp.int32)
    shifts = jnp.where(jnp.arange(N_ROW * N_COL, dtype=jnp.int32) == top_device, 0, shifts)
    live_count = jnp.right_shift(jnp.full((N_ROW * N_COL,), TILES_DEV, jnp.int32), shifts).reshape(N_ROW, N_COL)
    live_mask = jnp.arange(TILES_DEV, dtype=jnp.int32)[None, None, :] < live_count[:, :, None]
    row_ids = jnp.where(live_mask, chosen // SB, 0).astype(jnp.int32)
    col_ids = jnp.where(live_mask, chosen % SB, 0).astype(jnp.int32)
    return (row_ids, col_ids, live_count)


def draw_row_block(key, part):
    return tile_layout(key)[0]


def draw_col_block(key, part):
    return tile_layout(key)[1]


def draw_tile_count(key, part):
    return tile_layout(key)[2]


def block_scale(own_key, shape, cuts, low, top_value):
    gain = 1.0
    for dim, shards_of in cuts:
        draws = jax.random.uniform(jax.random.fold_in(jax.random.fold_in(own_key, 6), dim), (shards_of,), jnp.float32, low / len(cuts), top_value / len(cuts))
        gain = gain * jnp.repeat(jnp.exp(draws), shape[dim] // shards_of).reshape((-1,) + (1,) * (len(shape) - 1 - dim))
    return gain


def scatter_about(stream_key, extent, scale, limit, cuts=(), kind=jnp.bfloat16):
    gain = block_scale(stream_key, extent, cuts, -0.22, 0.18) if cuts else 1.0
    values = jax.random.normal(stream_key, extent, jnp.float32) * scale * gain
    return jnp.minimum(jnp.maximum(values, -limit), limit).astype(kind)


def setup_inputs(seed: int = 0) -> dict:
    streams_of = jax.random.split(jax.random.key(seed), 10)
    return {
        "node_features": scatter_about(streams_of[0], (NODES, F), 1.0, 6.0, ((0, 256),)),
        "src_norm": jnp.clip(jnp.exp(math.log(1.0) - 2.9957323 * jax.random.uniform(streams_of[1], (NODES,), jnp.float32) ** block_scale(streams_of[1], (NODES,), ((0, 256),), -0.2, 0.2)), 0.05, 1.0),
        "dst_norm": jnp.clip(jnp.exp(math.log(1.0) - 2.3025851 * jax.random.uniform(streams_of[2], (N_COL, DB * TB), jnp.float32) ** block_scale(streams_of[2], (N_COL, DB * TB), ((0, 16), (1, 16)), -0.2, 0.2)), 0.1, 1.0),
        "tiles": jnp.clip(0.049804688 * jax.random.uniform(streams_of[3], (N_ROW, N_COL, TILES_DEV, TB, TB), jnp.float32) ** block_scale(streams_of[3], (N_ROW, N_COL, TILES_DEV, TB, TB), ((0, 16), (1, 16)), -0.2, 0.2), 0.0, 0.049804688).astype(jnp.bfloat16),
        "row_block": draw_row_block(jax.random.fold_in(streams_of[9], 71), 0),
        "col_block": draw_col_block(jax.random.fold_in(streams_of[9], 71), 0),
        "tile_count": draw_tile_count(jax.random.fold_in(streams_of[9], 71), 0),
        "weight": scatter_about(streams_of[7], (F, F), F ** -0.5, 0.5),
        "bias": scatter_about(streams_of[8], (F,), 0.5, 3.0, (), jnp.float32),
    }


def device_sum(tile_set, row_ids, col_ids, live_count, blocks):
    live_mask = (jnp.arange(row_ids.shape[0], dtype=jnp.int32) < live_count).astype(jnp.float32)
    picked = blocks[col_ids]
    products = jnp.einsum("tij,tjf->tif", tile_set.astype(jnp.float32), picked.astype(jnp.float32), precision=lax.Precision.HIGHEST)
    products = products * live_mask[:, None, None]
    return jax.ops.segment_sum(products, row_ids, num_segments=DB)


def reference(node_features, src_norm, dst_norm, tiles, row_block, col_block, tile_count, weight, bias):
    scaled = (src_norm[:, None] * node_features.astype(jnp.float32)).astype(jnp.bfloat16)
    groups = scaled.reshape(N_ROW, SB, TB, F)

    def per_col(col_index):
        def add_device(running, row_index):
            part_sum = device_sum(tiles[row_index, col_index], row_block[row_index, col_index], col_block[row_index, col_index], tile_count[row_index, col_index], groups[row_index])
            rounded = lax.optimization_barrier(part_sum.astype(jnp.bfloat16))
            return running + rounded.astype(jnp.float32), None

        running, unused = lax.scan(add_device, jnp.zeros((DB, TB, F), jnp.float32), jnp.arange(N_ROW, dtype=jnp.int32))
        return running.reshape(DB * TB, F)

    aggregate = lax.map(per_col, jnp.arange(N_COL, dtype=jnp.int32))
    hidden = (dst_norm[..., None] * aggregate).astype(jnp.bfloat16)
    mixed = jnp.dot(hidden.reshape(-1, F), weight, preferred_element_type=jnp.float32) + bias
    return jnp.maximum(mixed, 0.0).astype(jnp.bfloat16).reshape(N_COL, DB * TB, F)
```

```python
import jax
import jax.numpy as jnp
from jax import lax
from jax.experimental import pallas as pl
from jax.experimental.pallas import tpu as pltpu
from jax.sharding import Mesh
from jax.sharding import PartitionSpec as P

COL = ("col_0", "col_1")
ROW_COL = ("row", "col_0", "col_1")
CHUNK = 16
GROUP = 4


def laid_out(pieces, dim):
    pieces = jnp.moveaxis(pieces, 0, dim)
    dims = pieces.shape
    return pieces.reshape(*dims[:dim], dims[dim] * dims[dim + 1], *dims[dim + 2 :])


def gather_in_order(shard, axes, turns):
    pieces = shard[None]
    for k in turns:
        pieces = lax.all_gather(pieces, axes[k], axis=0, tiled=True)
    block = [lax.axis_size(axes[k]) for k in reversed(turns)]
    pieces = pieces.reshape(*block, *shard.shape)
    turned = sorted(range(len(turns)), key=lambda place: turns[len(turns) - 1 - place])
    return pieces.transpose(*turned, *range(len(turns), pieces.ndim)).reshape(-1, *shard.shape)


def gathered_by_axis(shard, axes, turns, dim):
    return laid_out(gather_in_order(shard, axes, turns), dim)


def tile_sums(
    count_ref, row_ref, col_ref, feat_hbm, tiles_hbm, out_ref, feat, tiles, acc, tile_sem, feat_sem
):
    count = count_ref[0]
    dests = out_ref.shape[0]
    chunks = (count + CHUNK - 1) // CHUNK

    def tile_copy(k):
        span = pl.ds(pl.multiple_of(k * CHUNK, CHUNK), CHUNK)
        return pltpu.make_async_copy(tiles_hbm.at[span], tiles.at[span], tile_sem.at[k])

    feat_copy = pltpu.make_async_copy(feat_hbm, feat, feat_sem)
    feat_copy.start()

    @pl.loop(0, chunks)
    def _(k):
        tile_copy(k).start()

    @pl.loop(0, dests, unroll=4)
    def _(d):
        acc[d] = jnp.zeros(acc.shape[1:], acc.dtype)

    feat_copy.wait()

    @pl.loop(0, chunks)
    def _(k):
        tile_copy(k).wait()
        for first in range(0, CHUNK, GROUP):
            slots = [k * CHUNK + first + u for u in range(GROUP)]
            products = [
                jnp.dot(tiles[t], feat[col_ref[t]], preferred_element_type=jnp.float32)
                for t in slots
            ]
            for t, product in zip(slots, products):
                acc[jnp.where(t < count, row_ref[t], dests)] += product

    @pl.loop(0, dests, unroll=4)
    def _(d):
        out_ref[d] = acc[d].astype(out_ref.dtype)


def block_sparse_product(count, row_ids, col_ids, blocks, tiles, dests):
    slots, side, _ = tiles.shape
    width = blocks.shape[-1]
    return pl.pallas_call(
        tile_sums,
        out_shape=jax.ShapeDtypeStruct((dests, side, width), jnp.bfloat16),
        in_specs=[pl.BlockSpec(memory_space=pltpu.SMEM)] * 3
        + [pl.BlockSpec(memory_space=pl.ANY)] * 2,
        out_specs=pl.BlockSpec(memory_space=pltpu.VMEM),
        scratch_shapes=[
            pltpu.VMEM(blocks.shape, jnp.bfloat16),
            pltpu.VMEM(tiles.shape, jnp.bfloat16),
            pltpu.VMEM((dests + 1, side, width), jnp.float32),
            pltpu.SemaphoreType.DMA((slots // CHUNK,)),
            pltpu.SemaphoreType.DMA,
        ],
        compiler_params=pltpu.CompilerParams(vmem_limit_bytes=40 * 2**20),
        name="tile_sums",
    )(count, row_ids, col_ids, blocks, tiles)


def shards(
    node_features, src_norm, dst_norm, tiles, row_block, col_block, tile_count, weight, bias
):
    tile_size = tiles.shape[-1]
    feat_width = node_features.shape[1]
    scaled = (src_norm[:, None] * node_features.astype(jnp.float32)).astype(jnp.bfloat16)
    gathered = gathered_by_axis(scaled, COL, (0, 1), 0)
    blocks = gathered.reshape(-1, tile_size, feat_width)
    dest_blocks = dst_norm.shape[1] * lax.axis_size("row") // tile_size
    partial_sum = block_sparse_product(
        tile_count[0], row_block[0, 0], col_block[0, 0], blocks, tiles[0, 0], dest_blocks
    ).reshape(dest_blocks * tile_size, feat_width)
    aggregate = lax.psum_scatter(
        partial_sum, "row", scatter_dimension=0, tiled=True
    ).astype(jnp.float32)
    hidden = (dst_norm[0][:, None] * aggregate).astype(jnp.bfloat16)
    mixed = jnp.dot(hidden, weight, preferred_element_type=jnp.float32) + bias
    return jnp.maximum(mixed, 0.0).astype(jnp.bfloat16)[None]


def solution(mesh):
    torus = Mesh(mesh.devices.reshape(mesh.shape["row"], 2, 8), ("row", "col_0", "col_1"))
    in_specs = (
        P(ROW_COL, None),
        P(ROW_COL),
        P(COL, "row"),
        P("row", COL, None, None, None),
        P("row", COL, None),
        P("row", COL, None),
        P("row", COL),
        P(),
        P(),
    )
    out_specs = P(COL, "row", None)
    return jax.shard_map(
        shards, mesh=torus, in_specs=in_specs, out_specs=out_specs, check_vma=False
    )
```

```python
import jax
import jax.numpy as jnp
from jax import lax
from jax.experimental import pallas as pl
from jax.experimental.pallas import tpu as pltpu
from jax.sharding import Mesh
from jax.sharding import PartitionSpec as P


ROW = ("xl", "y", "core")
COL = ("xh", "z")
CHUNK = 16
GROUP = 4
BF16 = jnp.bfloat16
F32 = jnp.float32


def shifted(value, axis, by):
    n = lax.axis_size(axis)
    return lax.ppermute(value, axis, [(i, (i + by) % n) for i in range(n)])


def swapped(value, axis):
    return lax.ppermute(value, axis, [(0, 1), (1, 0)])


def gathered(own):
    half = own.shape[0] // 2
    found = {(0, 0, 0): (own, 0), (0, 0, 1): (own, half)}
    up = shifted(own, "z", 1)
    down = shifted(own, "z", -1)
    other_top = swapped(own[:half], "xh")
    other_low = swapped(own[half:], "xh")
    found[1, 0, 0] = (other_top, 0)
    found[1, 0, 1] = (other_low, 0)
    for step in (1, 2, 3):
        for dz, value in ((-step, up), (step, down)):
            found[0, dz, 0] = (value, 0)
            found[0, dz, 1] = (value, half)
            if step > 1:
                found[1, dz + (1 if dz < 0 else -1), 0] = (value, 2 * half)
        if step < 3:
            onward_up, onward_down = up, down
            if step == 1:
                onward_up = jnp.concatenate([up, other_top])
                onward_down = jnp.concatenate([down, other_top])
        else:
            onward_up = jnp.concatenate([up[:half], up[2 * half :]])
            onward_down = down[half:]
        lows = jnp.concatenate([up[half : 2 * half], down[half : 2 * half]])
        up = shifted(onward_up, "z", 1)
        down = shifted(onward_down, "z", -1)
        lows = swapped(lows, "xh")
        found[1, -step, 1] = (lows, 0)
        found[1, step, 1] = (lows, half)
    found[0, 4, 0] = (up, 0)
    found[0, 4, 1] = (down, 0)
    found[1, -3, 0] = (up, half)
    found[1, 3, 0] = (down, half)
    last = swapped(jnp.concatenate([up[:half], down[:half]]), "xh")
    found[1, 4, 0] = (last, 0)
    found[1, 4, 1] = (last, half)
    return found


def tile_sums(places, *refs):
    (place_ref, count_ref, row_ref, col_ref), refs = refs[:4], refs[4:]
    n = len(refs) - 9
    parts, tiles_hbm = refs[:n], refs[n]
    keep_a, send_a, keep_b, send_b = refs[n + 1 : n + 5]
    feat, tiles, acc, tile_sem = refs[n + 5 : n + 9]
    count = count_ref[0]
    dests = acc.shape[0] - 1
    chunks = (count + CHUNK - 1) // CHUNK
    xl, y, core, xh, z = (place_ref[i] for i in range(5))

    def tile_copy(k):
        span = pl.ds(pl.multiple_of(k * CHUNK, CHUNK), CHUNK)
        return pltpu.make_async_copy(tiles_hbm.at[span], tiles.at[span], tile_sem.at[k])

    @pl.loop(0, chunks)
    def _(k):
        tile_copy(k).start()

    for (dx, dz, half), (part, row) in places.items():
        block = ((xh ^ dx) * 8 + ((z + dz) & 7)) * 8 + half * 4
        for i in range(4):
            feat[block + i] = parts[part][row + i * 128 : row + (i + 1) * 128]

    @pl.loop(0, dests, unroll=4)
    def _(d):
        acc[d] = jnp.zeros(acc.shape[1:], acc.dtype)

    @pl.loop(0, chunks)
    def _(k):
        tile_copy(k).wait()
        for first in range(0, CHUNK, GROUP):
            slots = [k * CHUNK + first + u for u in range(GROUP)]
            products = [
                jnp.dot(tiles[t], feat[col_ref[t]], preferred_element_type=F32) for t in slots
            ]
            for t, product in zip(slots, products):
                acc[jnp.where(t < count, row_ref[t], dests)] += product

    @pl.loop(0, 2)
    def _(dx):
        @pl.loop(0, 4)
        def _(dy):
            for mine, (to_a, to_b) in ((0, (keep_a, keep_b)), (1, (send_a, send_b))):
                block = (((xl ^ dx) * 4 + ((y + dy) & 3)) * 2 + (core ^ mine)) * 8
                for i in range(4):
                    to_a[dx, dy, i] = acc[block + i].astype(BF16)
                    to_b[dy, dx, i] = acc[block + 4 + i].astype(BF16)


def block_sparse_product(place, count, row_ids, col_ids, found, tiles, dests):
    slots, side, width = tiles.shape
    parts = list({id(value): value for value, _ in found.values()}.values())
    index = {id(value): i for i, value in enumerate(parts)}
    places = {key: (index[id(value)], row) for key, (value, row) in found.items()}
    out_a = jax.ShapeDtypeStruct((2, 4, 4, side, width), BF16)
    out_b = jax.ShapeDtypeStruct((4, 2, 4, side, width), BF16)

    def kernel(*refs):
        tile_sums(places, *refs)

    return pl.pallas_call(
        kernel,
        out_shape=(out_a, out_a, out_b, out_b),
        in_specs=[pl.BlockSpec(memory_space=pltpu.SMEM)] * 4
        + [pl.BlockSpec(memory_space=pltpu.VMEM)] * len(parts)
        + [pl.BlockSpec(memory_space=pl.ANY)],
        out_specs=[pl.BlockSpec(memory_space=pltpu.VMEM)] * 4,
        scratch_shapes=[
            pltpu.VMEM((128, side, width), BF16),
            pltpu.VMEM(tiles.shape, BF16),
            pltpu.VMEM((dests + 1, side, width), F32),
            pltpu.SemaphoreType.DMA((slots // CHUNK,)),
        ],
        compiler_params=pltpu.CompilerParams(vmem_limit_bytes=40 * 2**20),
        name="tile_sums",
    )(place, count, row_ids, col_ids, *parts, tiles)


def added(*values):
    total = values[0].astype(F32)
    for value in values[1:]:
        total = total + value.astype(F32)
    return total


def scattered(keep_a, send_a, keep_b, send_b):
    got_a = swapped(send_a, "core")
    got_b = swapped(send_b, "core")
    far_a = swapped(added(keep_a[1], got_a[1]).astype(BF16), "xl")
    far_b = [shifted(added(keep_b[k], got_b[k]).astype(BF16), "y", k) for k in (1, 3, 2)]
    sum_a = added(keep_a[0], got_a[0], far_a)
    near_a = [shifted(sum_a[k].astype(BF16), "y", k) for k in (1, 3, 2)]
    sum_b = added(keep_b[0], got_b[0], *far_b)
    last_b = swapped(sum_b[1].astype(BF16), "xl")
    total_a = added(sum_a[0], *near_a)
    total_b = added(sum_b[0], last_b)
    return jnp.concatenate([total_a, total_b]).reshape(-1, keep_a.shape[-1])


def shards(
    node_features, src_norm, dst_norm, tiles, row_block, col_block, tile_count, weight, bias
):
    place = jnp.stack([lax.axis_index(a) for a in ROW + COL]).astype(jnp.int32)
    scaled = (src_norm[:, None] * node_features.astype(F32)).astype(BF16)
    found = gathered(scaled)
    dests = dst_norm.shape[1] * 16 // tiles.shape[-1]
    sums = block_sparse_product(
        place, tile_count[0], row_block[0, 0], col_block[0, 0], found, tiles[0, 0], dests
    )
    aggregate = scattered(*sums)
    hidden = (dst_norm[0][:, None] * aggregate).astype(BF16)
    mixed = jnp.dot(hidden, weight, preferred_element_type=F32) + bias
    return jnp.maximum(mixed, 0.0).astype(BF16)[None]


def solution(mesh):
    torus = Mesh(mesh.devices.reshape(2, 4, 2, 2, 8), ROW + COL)
    in_specs = (
        P(ROW + COL, None),
        P(ROW + COL),
        P(COL, ROW),
        P(ROW, COL, None, None, None),
        P(ROW, COL, None),
        P(ROW, COL, None),
        P(ROW, COL),
        P(),
        P(),
    )
    out_specs = P(COL, ROW, None)

    return jax.shard_map(
        shards, mesh=torus, in_specs=in_specs, out_specs=out_specs, check_vma=False
    )
```

```python
import jax
import jax.numpy as jnp
from jax import lax
from jax.experimental import pallas as pl
from jax.experimental.pallas import tpu as pltpu
from jax.sharding import Mesh
from jax.sharding import PartitionSpec as P


ROW = ("xl", "y", "core")
COL = ("xh", "z")
BF16 = jnp.bfloat16
F32 = jnp.float32


def swapped(value, axis, partner):
    n = lax.axis_size(axis)
    return lax.ppermute(value, axis, [(i, partner(i) % n) for i in range(n)])


def other(i):
    return i ^ 1


def other_side(i):
    return i + (i & 1) * 2 - 1


def gathered(own):
    half = own.shape[0] // 2
    found = {(0, 0, 0): (own, 0), (0, 0, 1): (own, half)}
    across = swapped(own, "xh", other)
    near = swapped(own, "z", other)
    back = swapped(own, "z", other_side)
    other_top = across[:half]
    found[1, 0, 0] = (across, 0)
    found[1, 0, 1] = (across, half)
    for step in (1, 2, 3):
        for sign, value in ((1, near), (-1, back)):
            found[0, sign * step, 0] = (value, 0)
            found[0, sign * step, 1] = (value, half)
            if step > 1:
                found[1, sign * (step - 1), 0] = (value, 2 * half)
        if step == 1:
            from_near = jnp.concatenate([near, other_top])
            from_back = jnp.concatenate([back, other_top])
        elif step == 2:
            from_near, from_back = near, back
        else:
            from_near = near[half:]
            from_back = jnp.concatenate([back[:half], back[2 * half :]])
        lows = jnp.concatenate([near[half : 2 * half], back[half : 2 * half]])
        near = swapped(from_back, "z", other)
        back = swapped(from_near, "z", other_side)
        lows = swapped(lows, "xh", other)
        found[1, step, 1] = (lows, 0)
        found[1, -step, 1] = (lows, half)
    found[0, 4, 0] = (near, 0)
    found[0, 4, 1] = (back, 0)
    found[1, 3, 0] = (near, half)
    found[1, -3, 0] = (back, half)
    last = swapped(jnp.concatenate([near[:half], back[:half]]), "xh", other)
    found[1, 4, 0] = (last, 0)
    found[1, 4, 1] = (last, half)
    return found


PHASES = 3
BLOCK = 16
STEP = 4
CAP = 320 + STEP
SHARES = (688, 336)
HALVINGS = ((("xl", 1, 3), (1, 3, "xl")), ((3, "xl", 1), (3, "xl", 1)))


def phase_of(key):
    dx, dz, half = key
    far = abs(dz)
    if not dx:
        return (0, 0, 0, 1, 1)[far]
    return ((0, 0, 1, 1, 2), (0, 0, 1, 2, 2))[half][far]


def place():
    z = lax.axis_index("z")
    return lax.axis_index("xh"), z, 1 - 2 * (z & 1)


def prepare(keys, count_ref, row_ref, col_ref, tiles_hbm, acc, codes, tiles, tile_sem):
    fetch = pltpu.make_async_copy(tiles_hbm.at[0, 0], tiles, tile_sem)
    fetch.start()
    zeros = jnp.zeros((128, acc.shape[1]), acc.dtype)

    @pl.loop(0, acc.shape[0] // 128)
    def _(d):
        acc[pl.ds(pl.multiple_of(d * 128, 128), 128)] = zeros

    count = count_ref[0, 0]
    xh, z, sign = place()
    flip = (sign - 1) >> 1
    start = z ^ flip
    tables = [0, 0]
    for dx, dz, half in keys:
        tables[dx] |= phase_of((dx, dz, half)) << ((dz & 7) * 4 + half * 2)
    tables = [jnp.int32(m - (1 << 32) if m >> 31 else m) for m in tables]
    near_table = jnp.where(xh == 0, tables[0], tables[1])
    far_table = jnp.where(xh == 0, tables[1], tables[0])

    def list_slots(k, counts):
        for u in range(STEP):
            t = k * STEP + u
            col = col_ref[0, 0, t]
            shift = ((((col >> 3) ^ flip) - start) & 7) * 4 + ((col >> 1) & 2)
            phase = (jnp.where(col < 64, near_table, far_table) >> shift) & 3
            field = phase * 10
            codes[phase * CAP + ((counts >> field) & 1023)] = (
                t | (row_ref[0, 0, t] << 9) | (col << 17)
            )
            counts = counts + ((((t - count) >> 31) & 1) << field)
        return counts

    counts = lax.fori_loop(0, (count + STEP - 1) // STEP, list_slots, jnp.int32(0))
    for p in range(PHASES):
        n = (counts >> (10 * p)) & 1023
        codes[PHASES * CAP + p] = n
        for i in range(STEP):
            codes[p * CAP + n + i] = jnp.int32((acc.shape[0] // 128 - 1) << 9)
    fetch.wait()


def prepared(keys, count, row_ids, col_ids, tiles, dests):
    side, width = tiles.shape[3:]

    def kernel(*refs):
        prepare(keys, *refs)

    smem, vmem = (pl.BlockSpec(memory_space=m) for m in (pltpu.SMEM, pltpu.VMEM))
    return pl.pallas_call(
        kernel,
        out_shape=(
            jax.ShapeDtypeStruct(((dests + 1) * side, width), F32),
            jax.ShapeDtypeStruct((PHASES * CAP + PHASES,), jnp.int32),
            jax.ShapeDtypeStruct(tiles.shape[2:], tiles.dtype),
        ),
        in_specs=[smem] * 3 + [pl.BlockSpec(memory_space=pltpu.HBM)],
        out_specs=(vmem, smem, vmem),
        scratch_shapes=[pltpu.SemaphoreType.DMA],
        compiler_params=pltpu.CompilerParams(vmem_limit_bytes=34 * 2**20),
        name="prepare",
    )(count, row_ids, col_ids, tiles)


def add_products(phase, places, codes, tiles, parts, feat, acc):
    xh, z, sign = place()
    for (dx, dz, half), (part, row) in places.items():
        block = ((xh ^ dx) * 8 + ((z + sign * dz) & 7)) * 8 + half * 4
        for i in range(4):
            feat[block + i] = parts[part][row + i * 128 : row + (i + 1) * 128]

    def run(first, size):
        for start in range(0, size, STEP):
            entries = [codes[phase * CAP + first + start + u] for u in range(STEP)]
            products = [
                jnp.dot(tiles[e & 511], feat[e >> 17], preferred_element_type=F32)
                for e in entries
            ]
            for e, product in zip(entries, products):
                acc[pl.ds(pl.multiple_of(((e >> 9) & 255) * 128, 128), 128)] += product

    count = codes[PHASES * CAP + phase]
    whole = count // BLOCK

    @pl.loop(0, whole)
    def _(k):
        run(k * BLOCK, BLOCK)

    @pl.loop(0, (count - whole * BLOCK + STEP - 1) // STEP)
    def _(k):
        run(whole * BLOCK + k * STEP, STEP)


def parts_of(found, phase):
    mine = {key: at for key, at in found.items() if phase_of(key) == phase}
    parts = list({id(value): value for value, _ in mine.values()}.values())
    index = {id(value): i for i, value in enumerate(parts)}
    return parts, {key: (index[id(value)], row) for key, (value, row) in mine.items()}


def phase_sums(phase, codes, tiles, acc, found):
    parts, places = parts_of(found, phase)
    n = len(parts)

    def kernel(codes_ref, tiles_ref, acc_in, *refs):
        add_products(phase, places, codes_ref, tiles_ref, refs[:n], refs[n + 1], refs[n])

    smem, vmem = (pl.BlockSpec(memory_space=m) for m in (pltpu.SMEM, pltpu.VMEM))
    return pl.pallas_call(
        kernel,
        out_shape=jax.ShapeDtypeStruct(acc.shape, acc.dtype),
        in_specs=[smem, vmem, vmem] + [vmem] * n,
        out_specs=vmem,
        scratch_shapes=[pltpu.VMEM((128, *tiles.shape[1:]), BF16)],
        input_output_aliases={2: 0},
        compiler_params=pltpu.CompilerParams(vmem_limit_bytes=16 * 2**20),
    )(codes, tiles, acc, *parts)


def write_part(acc, part, keep, send):
    xl, y, core = (lax.axis_index(a) for a in ROW)

    @pl.loop(0, 8)
    def _(at):
        bits = (at >> 2, (at >> 1) & 1, at & 1)
        for mine, out in ((0, keep), (1, send)):
            dest_core = core ^ mine
            turns = [dict(zip(kinds, bits)) for kinds in HALVINGS[part]]
            turn = {k: jnp.where(dest_core == 0, turns[0][k], turns[1][k]) for k in turns[0]}
            device = ((xl ^ turn["xl"]) * 4 + (y ^ turn[1] ^ (3 * turn[3]))) * 2 + dest_core
            row = device * sum(SHARES) + sum(SHARES[:part])
            rows = acc[pl.ds(pl.multiple_of(row, 16), SHARES[part])]
            out[at] = rows.astype(BF16)


def last_sums(codes, tiles, acc, found):
    phase = PHASES - 1
    parts, places = parts_of(found, phase)
    n = len(parts)
    side, width = tiles.shape[1:]

    def kernel(codes_ref, tiles_ref, acc_in, *refs):
        sums, keep, send, feat = refs[n:]
        add_products(phase, places, codes_ref, tiles_ref, refs[:n], feat, sums)
        write_part(sums, 0, keep, send)

    def rest(acc_ref, keep, send):
        write_part(acc_ref, 1, keep, send)

    smem, vmem = (pl.BlockSpec(memory_space=m) for m in (pltpu.SMEM, pltpu.VMEM))
    out_a = jax.ShapeDtypeStruct((8, SHARES[0], width), BF16)
    out_b = jax.ShapeDtypeStruct((8, SHARES[1], width), BF16)
    params = pltpu.CompilerParams(vmem_limit_bytes=16 * 2**20)
    acc, keep_a, send_a = pl.pallas_call(
        kernel,
        out_shape=(jax.ShapeDtypeStruct(acc.shape, acc.dtype), out_a, out_a),
        in_specs=[smem, vmem, vmem] + [vmem] * n,
        out_specs=(vmem, vmem, vmem),
        scratch_shapes=[pltpu.VMEM((128, side, width), BF16)],
        input_output_aliases={2: 0},
        compiler_params=params,
    )(codes, tiles, acc, *parts)
    keep_b, send_b = pl.pallas_call(
        rest,
        out_shape=(out_b, out_b),
        in_specs=[vmem],
        out_specs=(vmem, vmem),
        compiler_params=params,
        name="rest",
    )(acc)
    return keep_a, send_a, keep_b, send_b


def added(*values):
    total = values[0].astype(F32)
    for value in values[1:]:
        total = total + value.astype(F32)
    return total


def halved(value, part, step):
    def partner(i):
        xl, y, core = i >> 3, (i >> 1) & 3, i & 1
        kind = HALVINGS[part][core][step]
        return (((xl ^ 1) * 4 + y) if kind == "xl" else (xl * 4 + (y ^ kind))) * 2 + core

    return lax.ppermute(value, ROW, [(i, partner(i)) for i in range(16)])


def scattered(keep_a, send_a, keep_b, send_b):
    held = [[keep_a, swapped(send_a, "core", other)], [keep_b, swapped(send_b, "core", other)]]
    for step in range(3):
        size = 4 >> step
        came = [
            halved(added(*(v[size:] for v in values)).astype(BF16), part, step)
            for part, values in enumerate(held)
        ]
        held = [[v[:size] for v in values] + [new] for values, new in zip(held, came)]
    return jnp.concatenate([added(*values)[0] for values in held])


def shards(
    node_features, src_norm, dst_norm, tiles, row_block, col_block, tile_count, weight, bias
):
    scaled = (src_norm[:, None] * node_features.astype(F32)).astype(BF16)
    dests = dst_norm.shape[1] * 16 // tiles.shape[-1]
    found = gathered(scaled)
    acc, codes, held = prepared(
        list(found), tile_count, row_block, col_block, tiles, dests
    )
    for phase in range(PHASES - 1):
        acc = phase_sums(phase, codes, held, acc, found)
    sums = last_sums(codes, held, acc, found)
    aggregate = scattered(*sums)
    hidden = (dst_norm[0][:, None] * aggregate).astype(BF16)
    mixed = jnp.dot(hidden, weight, preferred_element_type=F32) + bias
    return jnp.maximum(mixed, 0.0).astype(BF16)[None]


def solution(mesh):
    torus = Mesh(mesh.devices.reshape(2, 4, 2, 2, 8), ROW + COL)
    in_specs = (
        P(ROW + COL, None),
        P(ROW + COL),
        P(COL, ROW),
        P(ROW, COL, None, None, None),
        P(ROW, COL, None),
        P(ROW, COL, None),
        P(ROW, COL),
        P(),
        P(),
    )
    out_specs = P(COL, ROW, None)

    return jax.shard_map(
        shards, mesh=torus, in_specs=in_specs, out_specs=out_specs, check_vma=False
    )
```

```python
import jax
import jax.numpy as jnp
from jax import lax
from jax.experimental import pallas as pl
from jax.experimental.pallas import tpu as pltpu
from jax.sharding import Mesh
from jax.sharding import PartitionSpec as P


ROW = ("xl", "y", "core")
COL = ("xh", "z")
BF16 = jnp.bfloat16
F32 = jnp.float32


def swapped(value, axis, partner):
    n = lax.axis_size(axis)
    return lax.ppermute(value, axis, [(i, partner(i) % n) for i in range(n)])


def other(i):
    return i ^ 1


def other_side(i):
    return i + (i & 1) * 2 - 1


def copied(*pieces):
    width = pieces[0][0].shape[1]
    total = sum(rows for _, _, rows in pieces)

    def kernel(*refs):
        to = 0
        for ref, (_, first, rows) in zip(refs, pieces):
            refs[-1][to : to + rows] = ref[first : first + rows]
            to += rows

    vmem = pl.BlockSpec(memory_space=pltpu.VMEM)
    return pl.pallas_call(
        kernel,
        out_shape=jax.ShapeDtypeStruct((total, width), BF16),
        in_specs=[vmem] * len(pieces),
        out_specs=vmem,
        compiler_params=pltpu.CompilerParams(vmem_limit_bytes=4 * 2**20),
        name="copied",
    )(*(value for value, _, _ in pieces))


def gathered(own):
    half = own.shape[0] // 2
    found = {(0, 0, 0): (own, 0), (0, 0, 1): (own, half)}
    near = swapped(own, "z", other)
    back = swapped(own, "z", other_side)
    other_top = swapped(copied((own, 0, half)), "xh", other)
    other_low = swapped(copied((own, half, half)), "xh", other)
    found[1, 0, 0] = (other_top, 0)
    found[1, 0, 1] = (other_low, 0)
    for step in (1, 2, 3):
        for sign, value in ((1, near), (-1, back)):
            found[0, sign * step, 0] = (value, 0)
            found[0, sign * step, 1] = (value, half)
            if step > 1:
                found[1, sign * (step - 1), 0] = (value, 2 * half)
        if step == 1:
            from_near = jnp.concatenate([near, other_top])
            from_back = jnp.concatenate([back, other_top])
        elif step == 2:
            from_near, from_back = near, back
        else:
            from_near = near[half:]
            from_back = jnp.concatenate([back[:half], back[2 * half :]])
        lows = copied((near, half, half), (back, half, half))
        near = swapped(from_back, "z", other)
        back = swapped(from_near, "z", other_side)
        lows = swapped(lows, "xh", other)
        found[1, step, 1] = (lows, 0)
        found[1, -step, 1] = (lows, half)
    found[0, 4, 0] = (near, 0)
    found[0, 4, 1] = (back, 0)
    found[1, 3, 0] = (near, half)
    found[1, -3, 0] = (back, half)
    last = swapped(copied((near, 0, half), (back, 0, half)), "xh", other)
    found[1, 4, 0] = (last, 0)
    found[1, 4, 1] = (last, half)
    return found


PHASES = 3
BLOCK = 16
STEP = 4
CAP = 320 + STEP
SHARES = (384, 640)
HALVINGS = (((3, "xl", 1), (3, "xl", 1)), ((1, 3, "xl"), ("xl", 1, 3)))


def phase_of(key):
    dx, dz, half = key
    far = abs(dz)
    if not dx:
        return (0, 0, 0, 1, 1)[far]
    return ((0, 0, 1, 1, 2), (0, 0, 1, 2, 2))[half][far]


def place():
    z = lax.axis_index("z")
    return lax.axis_index("xh"), z, 1 - 2 * (z & 1)


def prepare(keys, count_ref, row_ref, col_ref, tiles_hbm, acc, codes, tiles, tile_sem):
    fetch = pltpu.make_async_copy(tiles_hbm.at[0, 0], tiles, tile_sem)
    fetch.start()
    zeros = jnp.zeros((128, acc.shape[1]), acc.dtype)

    @pl.loop(0, acc.shape[0] // 128)
    def _(d):
        acc[pl.ds(pl.multiple_of(d * 128, 128), 128)] = zeros

    count = count_ref[0, 0]
    xh, z, sign = place()
    flip = (sign - 1) >> 1
    start = z ^ flip
    tables = [0, 0]
    for dx, dz, half in keys:
        tables[dx] |= phase_of((dx, dz, half)) << ((dz & 7) * 4 + half * 2)
    tables = [jnp.int32(m - (1 << 32) if m >> 31 else m) for m in tables]
    near_table = jnp.where(xh == 0, tables[0], tables[1])
    far_table = jnp.where(xh == 0, tables[1], tables[0])

    def list_slots(k, counts):
        for u in range(STEP):
            t = k * STEP + u
            col = col_ref[0, 0, t]
            shift = ((((col >> 3) ^ flip) - start) & 7) * 4 + ((col >> 1) & 2)
            phase = (jnp.where(col < 64, near_table, far_table) >> shift) & 3
            field = phase * 10
            codes[phase * CAP + ((counts >> field) & 1023)] = (
                t | (row_ref[0, 0, t] << 9) | (col << 17)
            )
            counts = counts + ((((t - count) >> 31) & 1) << field)
        return counts

    counts = lax.fori_loop(0, (count + STEP - 1) // STEP, list_slots, jnp.int32(0))
    for p in range(PHASES):
        n = (counts >> (10 * p)) & 1023
        codes[PHASES * CAP + p] = n
        for i in range(STEP):
            codes[p * CAP + n + i] = jnp.int32((acc.shape[0] // 128 - 1) << 9)
    fetch.wait()


def prepared(keys, count, row_ids, col_ids, tiles, dests):
    side, width = tiles.shape[3:]

    def kernel(*refs):
        prepare(keys, *refs)

    smem, vmem = (pl.BlockSpec(memory_space=m) for m in (pltpu.SMEM, pltpu.VMEM))
    return pl.pallas_call(
        kernel,
        out_shape=(
            jax.ShapeDtypeStruct(((dests + 1) * side, width), F32),
            jax.ShapeDtypeStruct((PHASES * CAP + PHASES,), jnp.int32),
            jax.ShapeDtypeStruct(tiles.shape[2:], tiles.dtype),
        ),
        in_specs=[smem] * 3 + [pl.BlockSpec(memory_space=pltpu.HBM)],
        out_specs=(vmem, smem, vmem),
        scratch_shapes=[pltpu.SemaphoreType.DMA],
        compiler_params=pltpu.CompilerParams(vmem_limit_bytes=34 * 2**20),
        name="prepare",
    )(count, row_ids, col_ids, tiles)


def add_products(phase, places, codes, tiles, parts, feat, acc):
    xh, z, sign = place()
    for (dx, dz, half), (part, row) in places.items():
        block = ((xh ^ dx) * 8 + ((z + sign * dz) & 7)) * 8 + half * 4
        for i in range(4):
            feat[block + i] = parts[part][row + i * 128 : row + (i + 1) * 128]

    def run(first, size):
        for start in range(0, size, STEP):
            entries = [codes[phase * CAP + first + start + u] for u in range(STEP)]
            products = [
                jnp.dot(tiles[e & 511], feat[e >> 17], preferred_element_type=F32)
                for e in entries
            ]
            for e, product in zip(entries, products):
                acc[pl.ds(pl.multiple_of(((e >> 9) & 255) * 128, 128), 128)] += product

    count = codes[PHASES * CAP + phase]
    whole = count // BLOCK

    @pl.loop(0, whole)
    def _(k):
        run(k * BLOCK, BLOCK)

    @pl.loop(0, (count - whole * BLOCK + STEP - 1) // STEP)
    def _(k):
        run(whole * BLOCK + k * STEP, STEP)


def parts_of(found, phase):
    mine = {key: at for key, at in found.items() if phase_of(key) == phase}
    parts = list({id(value): value for value, _ in mine.values()}.values())
    index = {id(value): i for i, value in enumerate(parts)}
    return parts, {key: (index[id(value)], row) for key, (value, row) in mine.items()}


def phase_sums(phase, codes, tiles, acc, found):
    parts, places = parts_of(found, phase)
    n = len(parts)

    def kernel(codes_ref, tiles_ref, acc_in, *refs):
        add_products(phase, places, codes_ref, tiles_ref, refs[:n], refs[n + 1], refs[n])

    smem, vmem = (pl.BlockSpec(memory_space=m) for m in (pltpu.SMEM, pltpu.VMEM))
    return pl.pallas_call(
        kernel,
        out_shape=jax.ShapeDtypeStruct(acc.shape, acc.dtype),
        in_specs=[smem, vmem, vmem] + [vmem] * n,
        out_specs=vmem,
        scratch_shapes=[pltpu.VMEM((128, *tiles.shape[1:]), BF16)],
        input_output_aliases={2: 0},
        compiler_params=pltpu.CompilerParams(vmem_limit_bytes=16 * 2**20),
    )(codes, tiles, acc, *parts)


def write_part(acc, part, keep, send):
    xl, y, core = (lax.axis_index(a) for a in ROW)

    @pl.loop(0, 8)
    def _(at):
        bits = (at >> 2, (at >> 1) & 1, at & 1)
        for mine, out in ((0, keep), (1, send)):
            dest_core = core ^ mine
            turns = [dict(zip(kinds, bits)) for kinds in HALVINGS[part]]
            turn = {k: jnp.where(dest_core == 0, turns[0][k], turns[1][k]) for k in turns[0]}
            device = ((xl ^ turn["xl"]) * 4 + (y ^ turn[1] ^ (3 * turn[3]))) * 2 + dest_core
            row = device * sum(SHARES) + sum(SHARES[:part])
            rows = acc[pl.ds(pl.multiple_of(row, 16), SHARES[part])]
            out[at] = rows.astype(BF16)


def last_sums(codes, tiles, acc, found):
    phase = PHASES - 1
    parts, places = parts_of(found, phase)
    n = len(parts)
    side, width = tiles.shape[1:]

    def kernel(codes_ref, tiles_ref, acc_in, *refs):
        sums, keep, send, feat = refs[n:]
        add_products(phase, places, codes_ref, tiles_ref, refs[:n], feat, sums)
        write_part(sums, 0, keep, send)

    def rest(acc_ref, keep, send):
        write_part(acc_ref, 1, keep, send)

    smem, vmem = (pl.BlockSpec(memory_space=m) for m in (pltpu.SMEM, pltpu.VMEM))
    out_a = jax.ShapeDtypeStruct((8, SHARES[0], width), BF16)
    out_b = jax.ShapeDtypeStruct((8, SHARES[1], width), BF16)
    params = pltpu.CompilerParams(vmem_limit_bytes=16 * 2**20)
    acc, keep_a, send_a = pl.pallas_call(
        kernel,
        out_shape=(jax.ShapeDtypeStruct(acc.shape, acc.dtype), out_a, out_a),
        in_specs=[smem, vmem, vmem] + [vmem] * n,
        out_specs=(vmem, vmem, vmem),
        scratch_shapes=[pltpu.VMEM((128, side, width), BF16)],
        input_output_aliases={2: 0},
        compiler_params=params,
    )(codes, tiles, acc, *parts)
    keep_b, send_b = pl.pallas_call(
        rest,
        out_shape=(out_b, out_b),
        in_specs=[vmem],
        out_specs=(vmem, vmem),
        compiler_params=params,
        name="rest",
    )(acc)
    return keep_a, send_a, keep_b, send_b


def added(*values):
    total = values[0].astype(F32)
    for value in values[1:]:
        total = total + value.astype(F32)
    return total


def halved(value, part, step):
    def partner(i):
        xl, y, core = i >> 3, (i >> 1) & 3, i & 1
        kind = HALVINGS[part][core][step]
        return (((xl ^ 1) * 4 + y) if kind == "xl" else (xl * 4 + (y ^ kind))) * 2 + core

    return lax.ppermute(value, ROW, [(i, partner(i)) for i in range(16)])


def scattered(keep_a, send_a, keep_b, send_b):
    held = [[keep_a, swapped(send_a, "core", other)], [keep_b, swapped(send_b, "core", other)]]
    for step in range(3):
        size = 4 >> step
        came = []
        for part, values in enumerate(held):
            leaving = added(*(v[size:] for v in values)).astype(BF16)
            came.append(halved(leaving, part, step))
        held = [[v[:size] for v in values] + [new] for values, new in zip(held, came)]
    return jnp.concatenate([added(*values)[0] for values in held])


def shards(
    node_features, src_norm, dst_norm, tiles, row_block, col_block, tile_count, weight, bias
):
    scaled = (src_norm[:, None] * node_features.astype(F32)).astype(BF16)
    dests = dst_norm.shape[1] * 16 // tiles.shape[-1]
    found = gathered(scaled)
    acc, codes, held = prepared(
        list(found), tile_count, row_block, col_block, tiles, dests
    )
    for phase in range(PHASES - 1):
        acc = phase_sums(phase, codes, held, acc, found)
    sums = last_sums(codes, held, acc, found)
    aggregate = scattered(*sums)
    hidden = (dst_norm[0][:, None] * aggregate).astype(BF16)
    mixed = jnp.dot(hidden, weight, preferred_element_type=F32) + bias
    return jnp.maximum(mixed, 0.0).astype(BF16)[None]


def solution(mesh):
    torus = Mesh(mesh.devices.reshape(2, 4, 2, 2, 8), ROW + COL)
    in_specs = (
        P(ROW + COL, None),
        P(ROW + COL),
        P(COL, ROW),
        P(ROW, COL, None, None, None),
        P(ROW, COL, None),
        P(ROW, COL, None),
        P(ROW, COL),
        P(),
        P(),
    )
    out_specs = P(COL, ROW, None)

    return jax.shard_map(
        shards, mesh=torus, in_specs=in_specs, out_specs=out_specs, check_vma=False
    )
```
